1024 devices in a mesh: lev: 2 (over core), lat: 32 (over y, z_hi), lon: 16 (over z_lo, x).
Axes of the slice: x: 4, y: 8, z: 16 (z_hi: 4, z_lo: 4; z = z_hi * 4 + z_lo), core: 2. Of those that a mesh axis runs over, the one named last changes fastest.
Arguments:
- grid: bfloat16 [4, 192, 384, 512], P('lev', 'lat', 'lon'), may hold values from -12 to 12
- w_qkv: bfloat16 [512, 1536], replicated, may hold values from -0.25 to 0.25
- w_proj: bfloat16 [512, 512], replicated, may hold values from -0.25 to 0.25
- w_up: bfloat16 [512, 2048], replicated, may hold values from -0.25 to 0.25
- w_down: bfloat16 [2048, 512], replicated, may hold values from -0.125 to 0.125
- logit_scale: float32 [8], replicated, may hold values from 3 to 24
- gain_attn: float32 [512], replicated, may hold values from 0.1 to 1.9
- gain_mlp: float32 [512], replicated, may hold values from 0.1 to 1.9
Outputs:
- updated: bfloat16 [4, 192, 384, 512], P('lev', 'lat', 'lon')
The draws below stay inside these ranges and needn't reach their ends.
All inputs are finite; a program needn't handle non-finite values.
Results may differ from the reference program's by a relative error of at most 0.01.
Values may be sent and summed in bfloat16 or wider, within the bound.
No kernel may reach another device: no remote copies, remote signals or barrier semaphores. Data moves between devices by JAX's collectives and lax.ppermute only.
A program may use at most 32 MiB of HBM per device.

```python
import math
import jax
import jax.numpy as jnp
from jax import lax

C = 512
HEADS = 8
FF = 2048
WA = 6
WO = 12
LEVELS = 4
NA = 192
NO = 384


def draw_grid(key, part):
    first = jax.random.fold_in(key, 11)
    base = jax.random.normal(first, (LEVELS, NA, NO, C), jnp.float32)
    values = base
    return jnp.clip(values, -12.0, 12.0).astype(jnp.bfloat16)


def noise(key, shape, deviation, bound, kind=jnp.bfloat16):
    values = deviation * jax.random.normal(key, shape, jnp.float32)
    return jnp.clip(values, min=-bound, max=bound).astype(kind)


def setup_inputs(seed: int = 0) -> dict:
    streams_of = jax.random.split(jax.random.key(seed), 9)
    grid = draw_grid(jax.random.fold_in(streams_of[8], 71), 0)
    w_qkv = noise(streams_of[1], (C, 3 * C), C ** -0.5, 0.25)
    w_proj = noise(streams_of[2], (C, C), C ** -0.5, 0.25)
    w_up = noise(streams_of[3], (C, FF), C ** -0.5, 0.25)
    w_down = noise(streams_of[4], (FF, C), FF ** -0.5, 0.125)
    logit_scale = jnp.clip(jnp.exp(jax.random.uniform(streams_of[5], (HEADS,), jnp.float32, math.log(3.0), math.log(24.0))), 3.0, 24.0)
    gain_attn = jnp.clip(1.0 + 0.18 * jax.random.normal(streams_of[6], (C,), jnp.float32), 0.1, 1.9)
    gain_mlp = jnp.clip(1.0 + 0.18 * jax.random.normal(streams_of[7], (C,), jnp.float32), 0.1, 1.9)
    return dict(grid=grid, w_qkv=w_qkv, w_proj=w_proj, w_up=w_up, w_down=w_down, logit_scale=logit_scale, gain_attn=gain_attn, gain_mlp=gain_mlp)


def layer_norm(values, gain):
    mean = lax.optimization_barrier(jnp.mean(values, axis=-1, keepdims=True))
    centred = values - mean
    spread = lax.optimization_barrier(jnp.mean(centred * centred, axis=-1, keepdims=True))
    return centred * lax.rsqrt(spread + 1e-05) * gain

def to_windows(values, depth):
    levels, rows, cols, width = values.shape
    shaped = values.reshape(levels // depth, depth, rows // WA, WA, cols // WO, WO, width)
    shaped = jnp.transpose(shaped, (0, 2, 4, 1, 3, 5, 6))
    return shaped.reshape(-1, depth * WA * WO, width)

def from_windows(values, depth, levels, rows, cols):
    width = values.shape[-1]
    shaped = values.reshape(levels // depth, rows // WA, cols // WO, depth, WA, WO, width)
    shaped = jnp.transpose(shaped, (0, 3, 1, 4, 2, 5, 6))
    return shaped.reshape(levels, rows, cols, width)

def attend(packed, region, logit_scale):
    count, span, triple = packed.shape
    width = triple // 3
    heads = logit_scale.shape[0]
    size = width // heads
    query = packed[..., :width].astype(jnp.float32).reshape(count, span, heads, size)
    keys = packed[..., width:2 * width].astype(jnp.float32).reshape(count, span, heads, size)
    values = packed[..., 2 * width:].astype(jnp.float32).reshape(count, span, heads, size)
    raw = jnp.einsum('bqhd,bkhd->bhqk', query, keys)
    q_scale = lax.rsqrt(lax.optimization_barrier(jnp.sum(query * query, axis=-1)) + 1e-06)
    k_scale = lax.rsqrt(lax.optimization_barrier(jnp.sum(keys * keys, axis=-1)) + 1e-06)
    scores = raw * logit_scale[None, :, None, None]
    scores = scores * jnp.transpose(q_scale, (0, 2, 1))[:, :, :, None]
    scores = scores * jnp.transpose(k_scale, (0, 2, 1))[:, :, None, :]
    same = region[:, None, :, None] == region[:, None, None, :]
    expd = jnp.where(same, jnp.exp(scores), jnp.zeros_like(scores))
    weights = (expd / lax.optimization_barrier(jnp.sum(expd, axis=-1, keepdims=True))).astype(jnp.bfloat16)
    mixed = jnp.einsum('bhqk,bkhd->bqhd', weights.astype(jnp.float32), values)
    return mixed.astype(jnp.bfloat16).reshape(count, span, width)

def finish(flat, mixed, w_proj, w_up, w_down, gain_attn, gain_mlp):
    attn_out = jnp.dot(mixed, w_proj, preferred_element_type=jnp.float32).astype(jnp.bfloat16)
    settled = (flat.astype(jnp.float32) + layer_norm(attn_out.astype(jnp.float32), gain_attn)).astype(jnp.bfloat16)
    hidden = jax.nn.gelu(jnp.dot(settled, w_up, preferred_element_type=jnp.float32), approximate=True).astype(jnp.bfloat16)
    down = jnp.dot(hidden, w_down, preferred_element_type=jnp.float32)
    return (settled.astype(jnp.float32) + layer_norm(down, gain_mlp)).astype(jnp.bfloat16)

def reference(grid, w_qkv, w_proj, w_up, w_down, logit_scale, gain_attn, gain_mlp):
    half_rows = WA // 2
    half_cols = WO // 2
    rolled = jnp.roll(grid, (-1, -half_rows, -half_cols), axis=(0, 1, 2))
    level_global = (jnp.arange(LEVELS, dtype=jnp.int32) + 1) % LEVELS
    level_region = (level_global + 1) // 2

    def one_row(row):
        slab = lax.dynamic_slice_in_dim(rolled, (row * WA).astype(jnp.int32), WA, 1)
        lat_global = (row * WA + jnp.arange(WA, dtype=jnp.int32) + half_rows) % NA
        lat_region = (lat_global >= half_rows).astype(jnp.int32)
        region = level_region[:, None, None] * 2 + lat_region[None, :, None] + jnp.zeros((LEVELS, WA, NO), jnp.int32)
        flat = slab.reshape(-1, C)
        packed = jnp.dot(flat, w_qkv, preferred_element_type=jnp.float32).astype(jnp.bfloat16)
        windows = to_windows(packed.reshape(LEVELS, WA, NO, 3 * C), 2)
        region_windows = to_windows(region[..., None], 2)[..., 0]
        mixed = attend(windows, region_windows, logit_scale)
        mixed = from_windows(mixed, 2, LEVELS, WA, NO).reshape(-1, C)
        result = finish(flat, mixed, w_proj, w_up, w_down, gain_attn, gain_mlp)
        return result.reshape(LEVELS, WA, NO, C)
    blocks = lax.map(one_row, jnp.arange(NA // WA, dtype=jnp.int32))
    result = jnp.transpose(blocks, (1, 0, 2, 3, 4)).reshape(LEVELS, NA, NO, C)
    return jnp.roll(result, (1, half_rows, half_cols), axis=(0, 1, 2))
```

```python
import functools
import math

import jax
import jax.numpy as jnp
import numpy as np
from jax import lax
from jax.experimental import pallas as pl
from jax.experimental.pallas import tpu as pltpu
from jax.sharding import PartitionSpec as P

WA = 6
WO = 12
LOG2E = 1.4426950408889634


def shift(array, axis, by):
    length = lax.axis_size(axis)
    return lax.ppermute(array, axis, [(i, (i + by) % length) for i in range(length)])


def swap(array, axis):
    length = lax.axis_size(axis)
    return lax.ppermute(array, axis, [(i, i ^ 1) for i in range(length)])


def edge_select(rows, cols):
    half = rows // 2
    edge = WO // 2
    own = rows * cols
    starts = (0, own, half * cols, own + half * cols)
    pick = np.zeros((2, 4, half, edge, 2 * own), np.float32)
    for side in range(2):
        for part in range(4):
            for row in range(half):
                for col in range(edge):
                    source = starts[part] + row * cols + col + side * (cols - edge)
                    pick[side, part, row, col, source] = 1
    return pick.reshape(2 * 4 * half * edge, 2 * own)


def key_table(rows, cols):
    half = rows // 2
    edge = WO // 2
    table = []
    for r in range(rows):
        for c in range(cols):
            table.append((r // half, (c + edge) // WO, 0))
    for h in range(2):
        for r in range(half):
            for c in range(cols):
                table.append((h, (c + edge) // WO, 1))
    for side in range(2):
        for part in range(4):
            for _ in range(half * edge):
                table.append((part // 2, side * (cols // WO), part % 2))
    return np.array(table, np.int32)


def edges_kernel(pick_ref, own_ref, above_ref, below_ref, left_ref, right_ref):
    levels = own_ref.shape[0]
    count = left_ref.shape[1]
    for level in range(levels):
        source = jnp.concatenate([own_ref[level], above_ref[level], below_ref[level]], 0)
        edges = jnp.dot(pick_ref[...], source, preferred_element_type=jnp.float32)
        edges = edges.astype(jnp.bfloat16)
        left_ref[level] = edges[:count]
        right_ref[level] = edges[count:]


def join_kernel(lev_ref, own_ref, above_ref, below_ref, left_ref, right_ref, alone_ref, paired_ref):
    lev = lev_ref[0]
    for level, out_ref in ((lev, alone_ref), (1 - lev, paired_ref)):
        at = 0
        for ref in (own_ref, above_ref, below_ref, left_ref, right_ref):
            count = ref.shape[1]
            out_ref[at : at + count, :] = ref[level]
            at += count


def layer_norm(values, gain):
    mean = jnp.mean(values, axis=-1, keepdims=True)
    centred = values - mean
    spread = jnp.mean(centred * centred, axis=-1, keepdims=True)
    return centred * lax.rsqrt(spread + 1e-05) * gain


def square_sums(values, heads_of):
    squares = values.astype(jnp.float32)
    squares = squares * squares
    high = squares.astype(jnp.bfloat16)
    low = (squares - high.astype(jnp.float32)).astype(jnp.bfloat16)
    return high, low


def contract_last(a, b):
    return lax.dot_general(a, b, (((1,), (1,)), ((), ())), preferred_element_type=jnp.float32)


def attend(query, keys, values, mask, logit, heads_of):
    count, width = query.shape
    heads = heads_of.shape[0]
    size = width // heads
    pair = 2 * size
    high, low = square_sums(query, heads_of)
    q_scale = contract_last(high, heads_of) + contract_last(low, heads_of)
    q_scale = lax.rsqrt(q_scale + 1e-06) * logit
    high, low = square_sums(keys, heads_of)
    k_scale = contract_last(heads_of, high) + contract_last(heads_of, low)
    k_scale = lax.rsqrt(k_scale + 1e-06)
    lane = lax.broadcasted_iota(jnp.int32, (count, pair), 1)
    ones = jnp.ones((keys.shape[0], pair), jnp.bfloat16)
    parts = []
    for p in range(heads // 2):
        q = query[:, p * pair : (p + 1) * pair]
        k = keys[:, p * pair : (p + 1) * pair]
        v = jnp.concatenate([values[:, p * pair : (p + 1) * pair], ones], 1)
        outs = []
        for side in range(2):
            h = 2 * p + side
            inside = (lane >= size) if side else (lane < size)
            raw = contract_last(jnp.where(inside, q, jnp.zeros_like(q)), k)
            scores = raw * q_scale[:, h : h + 1] * k_scale[h : h + 1, :]
            expd = (jnp.exp2(scores) * mask).astype(jnp.bfloat16)
            mixed = jnp.dot(expd, v, preferred_element_type=jnp.float32)
            outs.append(mixed[:, :pair] / mixed[:, pair:])
        parts.append(jnp.where(lane < size, outs[0], outs[1]).astype(jnp.bfloat16))
    return jnp.concatenate(parts, 1)


def block_kernel(
    lev_ref, alone_ref, paired_ref, other_ref, mask_ref, heads_ref, logit_ref,
    qkv_ref, proj_ref, up_ref, down_ref, gain_attn_ref, gain_mlp_ref,
    out_ref, kv_ref, mixed_ref,
):
    lev = lev_ref[0]
    width = proj_ref.shape[0]
    span = alone_ref.shape[0]
    own = mask_ref.shape[0]
    for i, ref in enumerate((alone_ref, paired_ref, other_ref)):
        kv = jnp.dot(ref[...], qkv_ref[:, width:], preferred_element_type=jnp.float32)
        kv_ref[i * span : (i + 1) * span, :] = kv.astype(jnp.bfloat16)
    mask = mask_ref[...]
    logit = logit_ref[...] * LOG2E
    heads_of = heads_ref[...]
    for i, (ref, first, last) in enumerate(((alone_ref, 0, span), (paired_ref, span, 3 * span))):
        query = jnp.dot(ref[:own, :], qkv_ref[:, :width], preferred_element_type=jnp.float32)
        keys = kv_ref[first:last, :width]
        values = kv_ref[first:last, width:]
        wide = mask if i == 0 else jnp.concatenate([mask, mask], 1)
        mixed_ref[i * own : (i + 1) * own, :] = attend(
            query.astype(jnp.bfloat16), keys, values, wide, logit, heads_of
        )
    attn_out = jnp.dot(mixed_ref[...], proj_ref[...], preferred_element_type=jnp.float32)
    attn_out = attn_out.astype(jnp.bfloat16).astype(jnp.float32)
    stream = jnp.concatenate([alone_ref[:own, :], paired_ref[:own, :]], 0).astype(jnp.float32)
    settled = (stream + layer_norm(attn_out, gain_attn_ref[...])).astype(jnp.bfloat16)
    hidden = jnp.dot(settled, up_ref[...], preferred_element_type=jnp.float32)
    hidden = jax.nn.gelu(hidden, approximate=True).astype(jnp.bfloat16)
    down = jnp.dot(hidden, down_ref[...], preferred_element_type=jnp.float32)
    result = settled.astype(jnp.float32) + layer_norm(down, gain_mlp_ref[...])
    result = result.astype(jnp.bfloat16)
    out_ref[lev] = result[:own]
    out_ref[1 - lev] = result[own:]


def in_vmem(count):
    return [pl.BlockSpec(memory_space=pltpu.VMEM)] * count


SCALAR = pl.BlockSpec(memory_space=pltpu.SMEM)


def per_device(grid, w_qkv, w_proj, w_up, w_down, logit_scale, gain_attn, gain_mlp):
    levels, rows, cols, width = grid.shape
    half = rows // 2
    edge = WO // 2
    own = rows * cols
    heads = logit_scale.shape[0]
    bf16 = jnp.bfloat16
    lev = lax.axis_index("lev").astype(jnp.int32).reshape(1)
    lat = lax.axis_index("lat")
    last = lax.axis_size("lat") - 1

    table = key_table(rows, cols)
    same = (table[:own, None, :2] == table[None, :, :2]).all(-1)
    upper = ((table[:, 0] == 0) & (table[:, 2] == 1)).astype(np.float32)
    lower = ((table[:, 0] == 1) & (table[:, 2] == 1)).astype(np.float32)
    open_keys = 1 - upper * (lat == 0) - lower * (lat == last)
    mask = jnp.asarray(same.astype(np.float32)) * open_keys[None, :]
    heads_of = np.repeat(np.eye(heads, dtype=np.float32), width // heads, axis=1)

    tokens = grid.reshape(levels, own, width)
    below = shift(tokens[:, : half * cols], "lat", -1)
    above = shift(tokens[:, half * cols :], "lat", 1)

    side = jax.ShapeDtypeStruct((levels, 4 * half * edge, width), bf16)
    left, right = pl.pallas_call(
        edges_kernel, out_shape=(side, side), in_specs=in_vmem(4), out_specs=tuple(in_vmem(2)),
        name="edges",
    )(jnp.asarray(edge_select(rows, cols), bf16), tokens, above, below)
    from_east = shift(left, "lon", -1)
    from_west = shift(right, "lon", 1)

    span = table.shape[0]
    flat = jax.ShapeDtypeStruct((span, width), bf16)
    alone, paired = pl.pallas_call(
        join_kernel, out_shape=(flat, flat), in_specs=[SCALAR] + in_vmem(5),
        out_specs=tuple(in_vmem(2)), name="join",
    )(lev, tokens, above, below, from_west, from_east)
    other = swap(paired, "lev")

    out = pl.pallas_call(
        block_kernel,
        out_shape=jax.ShapeDtypeStruct((levels, own, width), bf16),
        in_specs=[SCALAR] + in_vmem(12),
        out_specs=in_vmem(1)[0],
        scratch_shapes=[
            pltpu.VMEM((3 * span, 2 * width), bf16),
            pltpu.VMEM((levels * own, width), bf16),
        ],
        compiler_params=pltpu.CompilerParams(vmem_limit_bytes=48 << 20),
        name="block",
    )(
        lev, alone, paired, other, mask, jnp.asarray(heads_of, bf16), logit_scale.reshape(1, heads),
        w_qkv, w_proj, w_up, w_down, gain_attn.reshape(1, width), gain_mlp.reshape(1, width),
    )
    return out.reshape(levels, rows, cols, width)


def solution(mesh):
    placed = (P("lev", "lat", "lon", None), P(), P(), P(), P(), P(), P(), P())
    return jax.shard_map(
        per_device,
        mesh=mesh,
        in_specs=placed,
        out_specs=P("lev", "lat", "lon", None),
        check_vma=False,
    )
```

```python
import jax
import jax.numpy as jnp
import numpy as np
from jax import lax
from jax.experimental import pallas as pl
from jax.experimental.pallas import tpu as pltpu
from jax.sharding import PartitionSpec as P


WA = 6
WO = 12
EDGE = WO // 2
LOG2E = 1.4426950408889634
AXES = ("lev", "lat", "lon")


def send(array, target):
    sizes = [lax.axis_size(axis) for axis in AXES]
    route = []
    for lev in range(sizes[0]):
        for lat in range(sizes[1]):
            for lon in range(sizes[2]):
                at = [lev, lat, lon]
                to = [t % size for t, size in zip(target(lev, lat, lon), sizes)]
                flat = [(p[0] * sizes[1] + p[1]) * sizes[2] + p[2] for p in (at, to)]
                route.append(tuple(flat))
    return lax.ppermute(array, AXES, route)


def column_group(cols, first, last):
    own = [r * cols + c for r in range(WA) for c in range(first, last)]
    halo = [WA * cols + r * cols + c for r in range(WA) for c in range(first, last)]
    return own + halo


def one_hot(indices, size):
    table = np.zeros((len(indices), size), np.float32)
    for row, index in enumerate(indices):
        if index >= 0:
            table[row, index] = 1
    return jnp.asarray(table, jnp.bfloat16)


def gather_kernel(lev_ref, pick_ref, own_ref, first_ref, second_ref, alone_ref, paired_ref, west_ref, cross_ref):
    lev = lev_ref[0]
    kept = alone_ref.shape[0]
    edge = cross_ref.shape[0]
    for i, (level, out_ref) in enumerate(((lev, alone_ref), (1 - lev, paired_ref))):
        source = jnp.concatenate([own_ref[level], first_ref[level], second_ref[level]], 0)
        picked = jnp.dot(pick_ref[...], source, preferred_element_type=jnp.float32)
        picked = picked.astype(jnp.bfloat16)
        out_ref[...] = picked[:kept]
        west_ref[i * edge : (i + 1) * edge, :] = picked[kept:]
        if i == 1:
            cross_ref[...] = picked[kept:]


def load_kernel(*refs):
    count = len(refs) // 2
    sems = refs[-1]
    copies = [pltpu.make_async_copy(refs[i], refs[count + i], sems.at[i]) for i in range(count)]
    for copy in copies:
        copy.start()
    for copy in copies:
        copy.wait()


def load(*args):
    return pl.pallas_call(
        load_kernel,
        out_shape=tuple(jax.ShapeDtypeStruct(a.shape, a.dtype) for a in args),
        in_specs=[pl.BlockSpec(memory_space=pltpu.HBM)] * len(args),
        out_specs=(VMEM,) * len(args),
        scratch_shapes=[pltpu.SemaphoreType.DMA((len(args),))],
        compiler_params=pltpu.CompilerParams(vmem_limit_bytes=10 << 20),
        name="load",
    )(*(pltpu.with_memory_space_constraint(a, pltpu.HBM) for a in args))


def layer_norm(values, gain):
    mean = jnp.mean(values, axis=-1, keepdims=True)
    centred = values - mean
    spread = jnp.mean(centred * centred, axis=-1, keepdims=True)
    return centred * lax.rsqrt(spread + 1e-05) * gain


def split_squares(values):
    squares = values.astype(jnp.float32)
    squares = squares * squares
    high = squares.astype(jnp.bfloat16)
    low = (squares - high.astype(jnp.float32)).astype(jnp.bfloat16)
    return high, low


def contract_last(a, b):
    return lax.dot_general(a, b, (((1,), (1,)), ((), ())), preferred_element_type=jnp.float32)


def attend(query, keys, values, allowed, logit, heads_of):
    count, width = query.shape
    heads = heads_of.shape[0]
    size = width // heads
    pair = 2 * size
    high, low = split_squares(query)
    q_scale = contract_last(high, heads_of) + contract_last(low, heads_of)
    q_scale = lax.rsqrt(q_scale + 1e-06) * logit
    high, low = split_squares(keys)
    k_scale = contract_last(heads_of, high) + contract_last(heads_of, low)
    k_scale = lax.rsqrt(k_scale + 1e-06)
    lane = lax.broadcasted_iota(jnp.int32, (count, pair), 1)
    zero = jnp.zeros((count, pair), jnp.bfloat16)
    ones = jnp.ones((keys.shape[0], pair), jnp.bfloat16)
    parts = []
    for p in range(heads // 2):
        q = query[:, p * pair : (p + 1) * pair]
        k = keys[:, p * pair : (p + 1) * pair]
        v = jnp.concatenate([values[:, p * pair : (p + 1) * pair], ones], 1)
        both = jnp.concatenate([jnp.where(lane < size, q, zero), jnp.where(lane < size, zero, q)], 0)
        raw = contract_last(both, k)
        expd = []
        for side in range(2):
            h = 2 * p + side
            scores = raw[side * count : (side + 1) * count] * q_scale[:, h : h + 1] * k_scale[h : h + 1, :]
            expd.append((jnp.exp2(scores) * allowed).astype(jnp.bfloat16))
        mixed = jnp.dot(jnp.concatenate(expd, 0), v, preferred_element_type=jnp.float32)
        mixed = mixed[:, :pair] / mixed[:, pair:]
        parts.append(jnp.where(lane < size, mixed[:count], mixed[count:]).astype(jnp.bfloat16))
    return jnp.concatenate(parts, 1)


def allowed_keys(place_ref, queries, group, swapped):
    lev = place_ref[0]
    shape = (queries, 2 * queries)
    row = lax.broadcasted_iota(jnp.int32, shape, 0)
    col = lax.broadcasted_iota(jnp.int32, shape, 1)
    row = lax.rem(row, group)
    col = lax.rem(col, 2 * group)
    quarter = group // 2
    q_half = jnp.where(row < quarter, 0, 1)
    first = lev if swapped else 1 - lev
    k_half = jnp.where(col < quarter, 0, jnp.where(col < 2 * quarter, 1, jnp.where(col < 3 * quarter, first, 1 - first)))
    closed = jnp.where(k_half == 0, place_ref[1], place_ref[2])
    return jnp.where((q_half == k_half) & ((col < group) | (closed == 0)), 1.0, 0.0)


def run_windows(sources, query, place_ref, group, heads_ref, logit_ref, weights, kv_ref):
    qkv_ref, proj_ref, up_ref, down_ref, gain_attn_ref, gain_mlp_ref = weights
    width = proj_ref.shape[0]
    tokens = kv_ref.shape[0]
    span = tokens // 3
    count = span // 2
    kv = jnp.dot(sources, qkv_ref[:, width:], preferred_element_type=jnp.float32)
    kv_ref[...] = kv.astype(jnp.bfloat16)
    q = jnp.dot(query, qkv_ref[:, :width], preferred_element_type=jnp.float32).astype(jnp.bfloat16)
    own = allowed_keys(place_ref, count, group, False)
    other = allowed_keys(place_ref, count, group, True)
    logit = logit_ref[...] * LOG2E
    mixed = []
    for i, (first, last, allowed) in enumerate(((0, span, own), (span, tokens, jnp.concatenate([own, other], 1)))):
        keys = kv_ref[first:last, :width]
        values = kv_ref[first:last, width:]
        mixed.append(attend(q[i * count : (i + 1) * count], keys, values, allowed, logit, heads_ref[...]))
    mixed = jnp.concatenate(mixed, 0)
    attn_out = jnp.dot(mixed, proj_ref[...], preferred_element_type=jnp.float32)
    attn_out = attn_out.astype(jnp.bfloat16).astype(jnp.float32)
    settled = (query.astype(jnp.float32) + layer_norm(attn_out, gain_attn_ref[...])).astype(jnp.bfloat16)
    hidden = jnp.dot(settled, up_ref[...], preferred_element_type=jnp.float32)
    hidden = jax.nn.gelu(hidden, approximate=True).astype(jnp.bfloat16)
    down = jnp.dot(hidden, down_ref[...], preferred_element_type=jnp.float32)
    result = settled.astype(jnp.float32) + layer_norm(down, gain_mlp_ref[...])
    return result.astype(jnp.bfloat16)


def border_kernel(
    place_ref, alone_ref, paired_ref, other_ref, east_ref, cross_ref, pick_ref, back_ref, heads_ref, logit_ref,
    qkv_ref, proj_ref, up_ref, down_ref, gain_attn_ref, gain_mlp_ref, out_ref, return_ref, kv_ref,
):
    edge = cross_ref.shape[0]
    start = alone_ref.shape[0] - edge
    pieces = (
        alone_ref[start:, :], east_ref[:edge, :], paired_ref[start:, :], east_ref[edge:, :],
        other_ref[start:, :], cross_ref[...],
    )
    sources = jnp.concatenate(pieces, 0)
    query = [
        jnp.dot(pick_ref[...], sources[i * 2 * edge : (i + 1) * 2 * edge], preferred_element_type=jnp.float32)
        for i in range(2)
    ]
    query = jnp.concatenate(query, 0).astype(jnp.bfloat16)
    weights = (qkv_ref, proj_ref, up_ref, down_ref, gain_attn_ref, gain_mlp_ref)
    result = run_windows(sources, query, place_ref, edge // 2, heads_ref, logit_ref, weights, kv_ref)
    out_ref[...] = result
    back = jnp.dot(back_ref[...], result, preferred_element_type=jnp.float32)
    return_ref[...] = back.astype(jnp.bfloat16)


def middle_kernel(
    place_ref, alone_ref, paired_ref, other_ref, border_ref, middle_to_ref, border_to_ref, heads_ref, logit_ref,
    qkv_ref, proj_ref, up_ref, down_ref, gain_attn_ref, gain_mlp_ref, out_ref, kv_ref,
):
    lev = place_ref[0]
    span = kv_ref.shape[0] // 3
    count = span // 2
    sources = jnp.concatenate([alone_ref[:span, :], paired_ref[:span, :], other_ref[:span, :]], 0)
    query = jnp.concatenate([alone_ref[:count, :], paired_ref[:count, :]], 0)
    weights = (qkv_ref, proj_ref, up_ref, down_ref, gain_attn_ref, gain_mlp_ref)
    result = run_windows(sources, query, place_ref, count, heads_ref, logit_ref, weights, kv_ref)
    for i, level in enumerate((lev, 1 - lev)):
        placed = jnp.dot(middle_to_ref[...], result[i * count : (i + 1) * count], preferred_element_type=jnp.float32)
        placed += jnp.dot(border_to_ref[...], border_ref[i * count : (i + 1) * count, :], preferred_element_type=jnp.float32)
        out_ref[level] = placed.astype(jnp.bfloat16)


def place_kernel(place_ref, partial_ref, returned_ref, returned_to_ref, out_ref):
    lev = place_ref[0]
    own = partial_ref.shape[1]
    for i, level in enumerate((lev, 1 - lev)):
        placed = jnp.dot(
            returned_to_ref[i * own : (i + 1) * own, :], returned_ref[...], preferred_element_type=jnp.float32
        )
        row = lax.broadcasted_iota(jnp.int32, placed.shape, 0)
        mine = lax.rem(row, own // WA) >= EDGE
        out_ref[level] = jnp.where(mine, partial_ref[level], placed.astype(jnp.bfloat16))


VMEM = pl.BlockSpec(memory_space=pltpu.VMEM)
SMEM = pl.BlockSpec(memory_space=pltpu.SMEM)


def call(kernel, outs, megabytes, scratch=()):
    def run(place, *args):
        return pl.pallas_call(
            kernel,
            out_shape=outs,
            in_specs=[SMEM] + [VMEM] * len(args),
            out_specs=jax.tree.map(lambda _: VMEM, outs),
            scratch_shapes=list(scratch),
            compiler_params=pltpu.CompilerParams(vmem_limit_bytes=megabytes << 20),
        )(place, *args)

    return run


def per_device(grid, w_qkv, w_proj, w_up, w_down, logit_scale, gain_attn, gain_mlp):
    levels, rows, cols, width = grid.shape
    own = rows * cols
    half = own // 2
    edge = 2 * WA * EDGE
    heads = logit_scale.shape[0]
    bf16 = jnp.bfloat16

    def shape(*dims):
        return jax.ShapeDtypeStruct(dims, bf16)

    lev = lax.axis_index("lev").astype(jnp.int32)
    lat = lax.axis_index("lat")
    last = lax.axis_size("lat") - 1
    place = jnp.stack([lev, (lat == 0).astype(jnp.int32), (lat == last).astype(jnp.int32)])

    tokens = grid.reshape(levels, own, width)
    halves = grid.reshape(levels, 2, half, width)
    sent_first = lax.dynamic_index_in_dim(halves, lev, 1, keepdims=False)
    sent_second = lax.dynamic_index_in_dim(halves, 1 - lev, 1, keepdims=False)
    first = send(sent_first, lambda c, i, j: (c, i + 2 * c - 1, j))
    second = send(sent_second, lambda c, i, j: (c, i + 1 - 2 * c, j))

    groups = column_group(cols, EDGE, EDGE + WO) + column_group(cols, EDGE + WO, cols) + column_group(cols, 0, EDGE)
    heads_of = jnp.asarray(np.repeat(np.eye(heads, dtype=np.float32), width // heads, axis=1), bf16)
    quarter = edge // 2
    spots = [(r, c) for r in range(rows) for c in range(cols)]
    pick = [edge + t for t in range(quarter)] + list(range(quarter))
    back = [i * edge + t for i in range(2) for t in range(quarter)]
    middle_to = [r * WO + c - EDGE if EDGE <= c < EDGE + WO else -1 for r, c in spots]
    border_to = [quarter + r * EDGE + c - EDGE - WO if c >= EDGE + WO else -1 for r, c in spots]
    returned_to = [i * quarter + r * EDGE + c if c < EDGE else -1 for i in range(2) for r, c in spots]
    tokens, groups, pick, back, middle_to, border_to, returned_to, *shared = load(
        tokens, one_hot(groups, 2 * own), one_hot(pick, 2 * edge), one_hot(back, 2 * edge), one_hot(middle_to, edge),
        one_hot(border_to, edge), one_hot(returned_to, edge),
        heads_of, logit_scale.reshape(1, heads), w_qkv, w_proj, w_up, w_down,
        gain_attn.reshape(1, width), gain_mlp.reshape(1, width),
    )

    kept = 2 * own - edge
    outs = (shape(kept, width), shape(kept, width), shape(2 * edge, width), shape(edge, width))
    alone, paired, west, west_paired = call(gather_kernel, outs, 8)(place, groups, tokens, first, second)
    east = send(west, lambda c, i, j: (c, i, j - 1))
    cross = send(west_paired, lambda c, i, j: (1 - c, i, j - 1))
    other = send(paired, lambda c, i, j: (1 - c, i, j))

    kv = [pltpu.VMEM((6 * edge, 2 * width), bf16)]
    border, returning = call(border_kernel, (shape(2 * edge, width), shape(edge, width)), 16, kv)(
        place, alone, paired, other, east, cross, pick, back, *shared
    )
    returned = send(returning, lambda c, i, j: (c, i, j + 1))
    partial = call(middle_kernel, shape(levels, own, width), 16, kv)(
        place, alone, paired, other, border, middle_to, border_to, *shared
    )
    out = call(place_kernel, shape(levels, own, width), 8)(place, partial, returned, returned_to)
    return out.reshape(levels, rows, cols, width)


def solution(mesh):
    placed = (P("lev", "lat", "lon", None), P(), P(), P(), P(), P(), P(), P())
    return jax.shard_map(
        per_device,
        mesh=mesh,
        in_specs=placed,
        out_specs=P("lev", "lat", "lon", None),
        check_vma=False,
    )
```

```python
import jax
import jax.numpy as jnp
import numpy as np
from jax import lax
from jax.experimental import pallas as pl
from jax.experimental.pallas import tpu as pltpu
from jax.sharding import PartitionSpec as P


WA = 6
WO = 12
HALF = WA // 2
EDGE = WO // 2
LOG2E = 1.4426950408889634
AXES = ("lev", "lat", "lon")


def send(array, target):
    sizes = [lax.axis_size(axis) for axis in AXES]
    route = []
    for lev in range(sizes[0]):
        for lat in range(sizes[1]):
            for lon in range(sizes[2]):
                at = [lev, lat, lon]
                to = [t % size for t, size in zip(target(lev, lat, lon), sizes)]
                flat = [(p[0] * sizes[1] + p[1]) * sizes[2] + p[2] for p in (at, to)]
                route.append(tuple(flat))
    return lax.ppermute(array, AXES, route)


def one_hot(indices, size):
    table = np.zeros((len(indices), size), np.float32)
    for row, index in enumerate(indices):
        if index >= 0:
            table[row, index] = 1
    return table


def padded(indices, size):
    return indices + [-1] * (size - len(indices))


def block(cols, level, first_row, rows, first_col, last_col):
    return [(level * WA + r) * cols + c for r in range(first_row, first_row + rows) for c in range(first_col, last_col)]


def rounded(size):
    return -(-size // 8) * 8


def split_picks(levels, cols):
    side = rounded(HALF * (cols - EDGE))
    corner = rounded(levels * HALF * EDGE)
    picks = []
    for lev in range(2):
        rows = []
        for start in (HALF * lev, HALF * (1 - lev)):
            for level in range(levels):
                rows += padded(block(cols, level, start, HALF, EDGE, cols), side)
        for start in (HALF * lev, HALF * (1 - lev)):
            rows += padded([t for level in range(levels) for t in block(cols, level, start, HALF, 0, EDGE)], corner)
        rows += [t for level in range(levels) for t in block(cols, level, 0, WA, 0, EDGE)]
        picks.append(one_hot(rows, levels * WA * cols))
    return np.stack(picks)


def gather_picks(levels, cols):
    own = WA * cols
    wide = cols - EDGE
    side = rounded(HALF * wide)
    corner = rounded(levels * HALF * EDGE)
    first, second = own, own + side
    corners = own + 2 * side
    east = corners + 2 * corner
    picks = []
    for level in range(levels):
        def halo(first_col, last_col):
            return [at + r * wide + c for at in (first, second) for r in range(HALF) for c in range(first_col, last_col)]

        cells = HALF * EDGE
        rows = block(cols, 0, 0, WA, EDGE, EDGE + WO) + halo(0, WO)
        rows += [east + level * 2 * cells + t for t in range(2 * cells)]
        rows += block(cols, 0, 0, WA, EDGE + WO, cols) + halo(WO, wide)
        rows += [corners + which * corner + level * cells + t for which in range(2) for t in range(cells)]
        picks.append(one_hot(rows, east + levels * 2 * cells))
    return np.stack(picks)


def split_kernel(lev_ref, pick_ref, grid_ref, own_ref, first_ref, second_ref, corner_ref, corner_2_ref, west_ref, held, sems):
    copies = [
        pltpu.make_async_copy(grid_ref, own_ref, sems.at[0]),
        pltpu.make_async_copy(pick_ref.at[lev_ref[0]], held, sems.at[1]),
    ]
    for copy in copies:
        copy.start()
    for copy in copies:
        copy.wait()
    levels, own, width = own_ref.shape
    picked = jnp.dot(held[...], own_ref[...].reshape(levels * own, width), preferred_element_type=jnp.float32)
    picked = picked.astype(jnp.bfloat16)
    at = 0
    for ref in (first_ref, second_ref):
        for level in range(levels):
            ref[level] = picked[at : at + ref.shape[1]]
            at += ref.shape[1]
    for ref in (corner_ref, corner_2_ref, west_ref):
        ref[...] = picked[at : at + ref.shape[0]]
        at += ref.shape[0]


def gather_kernel(lev_ref, pick_ref, own_ref, first_ref, second_ref, corner_ref, corner_2_ref, east_ref, alone_ref, paired_ref):
    lev = lev_ref[0]
    for level, out_ref in ((lev, alone_ref), (1 - lev, paired_ref)):
        source = [own_ref[level], first_ref[level], second_ref[level], corner_ref[...], corner_2_ref[...], east_ref[...]]
        picked = jnp.dot(pick_ref[level], jnp.concatenate(source, 0), preferred_element_type=jnp.float32)
        out_ref[...] = picked.astype(jnp.bfloat16)


def load_kernel(*refs):
    count = len(refs) // 2
    sems = refs[-1]
    copies = [pltpu.make_async_copy(refs[i], refs[count + i], sems.at[i]) for i in range(count)]
    for copy in copies:
        copy.start()
    for copy in copies:
        copy.wait()


def load(*args):
    return pl.pallas_call(
        load_kernel,
        out_shape=tuple(jax.ShapeDtypeStruct(a.shape, a.dtype) for a in args),
        in_specs=[pl.BlockSpec(memory_space=pltpu.HBM)] * len(args),
        out_specs=(VMEM,) * len(args),
        scratch_shapes=[pltpu.SemaphoreType.DMA((len(args),))],
        compiler_params=pltpu.CompilerParams(vmem_limit_bytes=10 << 20),
        name="load",
    )(*(pltpu.with_memory_space_constraint(a, pltpu.HBM) for a in args))


def layer_norm(values, gain):
    mean = jnp.mean(values, axis=-1, keepdims=True)
    centred = values - mean
    spread = jnp.mean(centred * centred, axis=-1, keepdims=True)
    return centred * lax.rsqrt(spread + 1e-05) * gain


def split_squares(values):
    squares = values.astype(jnp.float32)
    squares = squares * squares
    high = squares.astype(jnp.bfloat16)
    low = (squares - high.astype(jnp.float32)).astype(jnp.bfloat16)
    return high, low


def contract_last(a, b):
    return lax.dot_general(a, b, (((1,), (1,)), ((), ())), preferred_element_type=jnp.float32)


def attend(query, keys, values, allowed, logit, heads_of):
    count, width = query.shape
    heads = heads_of.shape[0]
    size = width // heads
    pair = 2 * size
    high, low = split_squares(query)
    q_scale = contract_last(high, heads_of) + contract_last(low, heads_of)
    q_scale = lax.rsqrt(q_scale + 1e-06) * logit
    high, low = split_squares(keys)
    k_scale = contract_last(heads_of, high) + contract_last(heads_of, low)
    k_scale = lax.rsqrt(k_scale + 1e-06)
    lane = lax.broadcasted_iota(jnp.int32, (count, pair), 1)
    zero = jnp.zeros((count, pair), jnp.bfloat16)
    ones = jnp.ones((keys.shape[0], pair), jnp.bfloat16)
    parts = []
    for p in range(heads // 2):
        q = query[:, p * pair : (p + 1) * pair]
        k = keys[:, p * pair : (p + 1) * pair]
        v = jnp.concatenate([values[:, p * pair : (p + 1) * pair], ones], 1)
        both = jnp.concatenate([jnp.where(lane < size, q, zero), jnp.where(lane < size, zero, q)], 0)
        raw = contract_last(both, k)
        expd = []
        for side in range(2):
            h = 2 * p + side
            scores = raw[side * count : (side + 1) * count] * q_scale[:, h : h + 1] * k_scale[h : h + 1, :]
            expd.append((jnp.exp2(scores) * allowed).astype(jnp.bfloat16))
        mixed = jnp.dot(jnp.concatenate(expd, 0), v, preferred_element_type=jnp.float32)
        mixed = mixed[:, :pair] / mixed[:, pair:]
        parts.append(jnp.where(lane < size, mixed[:count], mixed[count:]).astype(jnp.bfloat16))
    return jnp.concatenate(parts, 1)


def allowed_keys(place_ref, queries, period, swapped):
    lev = place_ref[0]
    shape = (queries, 2 * queries)
    row = lax.broadcasted_iota(jnp.int32, shape, 0)
    col = lax.broadcasted_iota(jnp.int32, shape, 1)
    q_half = jnp.where(lax.rem(row, period) < period // 2, 0, 1)
    part = jnp.where(lax.rem(col, period) < period // 2, 0, 1)
    first = lev if swapped else 1 - lev
    k_half = jnp.where(col < queries, part, jnp.where(part == 0, first, 1 - first))
    closed = jnp.where(k_half == 0, place_ref[1], place_ref[2])
    return jnp.where((q_half == k_half) & ((col < queries) | (closed == 0)), 1.0, 0.0)


def run_windows(sources, query, place_ref, period, heads_ref, logit_ref, weights, kv_ref):
    qkv_ref, proj_ref, up_ref, down_ref, gain_attn_ref, gain_mlp_ref = weights
    width = proj_ref.shape[0]
    tokens = kv_ref.shape[0]
    span = tokens // 3
    count = span // 2
    kv = jnp.dot(sources, qkv_ref[:, width:], preferred_element_type=jnp.float32)
    kv_ref[...] = kv.astype(jnp.bfloat16)
    q = jnp.dot(query, qkv_ref[:, :width], preferred_element_type=jnp.float32).astype(jnp.bfloat16)
    own = allowed_keys(place_ref, count, period, False)
    other = allowed_keys(place_ref, count, period, True)
    logit = logit_ref[...] * LOG2E
    mixed = []
    for i, (first, last, allowed) in enumerate(((0, span, own), (span, tokens, jnp.concatenate([own, other], 1)))):
        keys = kv_ref[first:last, :width]
        values = kv_ref[first:last, width:]
        mixed.append(attend(q[i * count : (i + 1) * count], keys, values, allowed, logit, heads_ref[...]))
    mixed = jnp.concatenate(mixed, 0)
    attn_out = jnp.dot(mixed, proj_ref[...], preferred_element_type=jnp.float32)
    attn_out = attn_out.astype(jnp.bfloat16).astype(jnp.float32)
    settled = (query.astype(jnp.float32) + layer_norm(attn_out, gain_attn_ref[...])).astype(jnp.bfloat16)
    hidden = jnp.dot(settled, up_ref[...], preferred_element_type=jnp.float32)
    hidden = jax.nn.gelu(hidden, approximate=True).astype(jnp.bfloat16)
    down = jnp.dot(hidden, down_ref[...], preferred_element_type=jnp.float32)
    result = settled.astype(jnp.float32) + layer_norm(down, gain_mlp_ref[...])
    return result.astype(jnp.bfloat16)


def border_kernel(
    place_ref, alone_ref, paired_ref, other_ref, back_ref, heads_ref, logit_ref,
    qkv_ref, proj_ref, up_ref, down_ref, gain_attn_ref, gain_mlp_ref, out_ref, return_ref, kv_ref,
):
    span = kv_ref.shape[0] // 3
    count = span // 2
    sources = jnp.concatenate([alone_ref[span:, :], paired_ref[span:, :], other_ref[span:, :]], 0)
    query = jnp.concatenate([alone_ref[span : span + count, :], paired_ref[span : span + count, :]], 0)
    weights = (qkv_ref, proj_ref, up_ref, down_ref, gain_attn_ref, gain_mlp_ref)
    result = run_windows(sources, query, place_ref, count // 2, heads_ref, logit_ref, weights, kv_ref)
    out_ref[...] = result
    back = jnp.dot(back_ref[...], result, preferred_element_type=jnp.float32)
    return_ref[...] = back.astype(jnp.bfloat16)


def middle_kernel(
    place_ref, alone_ref, paired_ref, other_ref, border_ref, middle_to_ref, border_to_ref, heads_ref, logit_ref,
    qkv_ref, proj_ref, up_ref, down_ref, gain_attn_ref, gain_mlp_ref, out_ref, kv_ref,
):
    lev = place_ref[0]
    span = kv_ref.shape[0] // 3
    count = span // 2
    sources = jnp.concatenate([alone_ref[:span, :], paired_ref[:span, :], other_ref[:span, :]], 0)
    query = jnp.concatenate([alone_ref[:count, :], paired_ref[:count, :]], 0)
    weights = (qkv_ref, proj_ref, up_ref, down_ref, gain_attn_ref, gain_mlp_ref)
    result = run_windows(sources, query, place_ref, count, heads_ref, logit_ref, weights, kv_ref)
    for i, level in enumerate((lev, 1 - lev)):
        placed = jnp.dot(middle_to_ref[...], result[i * count : (i + 1) * count], preferred_element_type=jnp.float32)
        placed += jnp.dot(border_to_ref[...], border_ref[i * count : (i + 1) * count, :], preferred_element_type=jnp.float32)
        out_ref[level] = placed.astype(jnp.bfloat16)


def place_kernel(place_ref, partial_ref, returned_ref, returned_to_ref, out_ref):
    lev = place_ref[0]
    own = partial_ref.shape[1]
    for i, level in enumerate((lev, 1 - lev)):
        placed = jnp.dot(
            returned_to_ref[i * own : (i + 1) * own, :], returned_ref[...], preferred_element_type=jnp.float32
        )
        row = lax.broadcasted_iota(jnp.int32, placed.shape, 0)
        mine = lax.rem(row, own // WA) >= EDGE
        out_ref[level] = jnp.where(mine, partial_ref[level], placed.astype(jnp.bfloat16))


VMEM = pl.BlockSpec(memory_space=pltpu.VMEM)
SMEM = pl.BlockSpec(memory_space=pltpu.SMEM)


def call(kernel, outs, megabytes, scratch=()):
    def run(place, *args):
        return pl.pallas_call(
            kernel,
            out_shape=outs,
            in_specs=[SMEM] + [VMEM] * len(args),
            out_specs=jax.tree.map(lambda _: VMEM, outs),
            scratch_shapes=list(scratch),
            compiler_params=pltpu.CompilerParams(vmem_limit_bytes=megabytes << 20),
        )(place, *args)

    return run


def per_device(grid, w_qkv, w_proj, w_up, w_down, logit_scale, gain_attn, gain_mlp):
    levels, rows, cols, width = grid.shape
    own = rows * cols
    edge = 2 * WA * EDGE
    heads = logit_scale.shape[0]
    bf16 = jnp.bfloat16

    def shape(*dims):
        return jax.ShapeDtypeStruct(dims, bf16)

    lev = lax.axis_index("lev").astype(jnp.int32)
    lat = lax.axis_index("lat")
    last = lax.axis_size("lat") - 1
    place = jnp.stack([lev, (lat == 0).astype(jnp.int32), (lat == last).astype(jnp.int32)])

    side = rounded(HALF * (cols - EDGE))
    corner = rounded(levels * HALF * EDGE)
    outs = (
        shape(levels, own, width), shape(levels, side, width), shape(levels, side, width),
        shape(corner, width), shape(corner, width), shape(edge, width),
    )
    picks = split_picks(levels, cols)
    in_hbm = pl.BlockSpec(memory_space=pltpu.HBM)
    held = [pltpu.VMEM(picks.shape[1:], bf16), pltpu.SemaphoreType.DMA((2,))]
    tokens, first, second, corner_1, corner_2, west = pl.pallas_call(
        split_kernel, out_shape=outs, in_specs=[SMEM, in_hbm, in_hbm], out_specs=(VMEM,) * len(outs), scratch_shapes=held,
        compiler_params=pltpu.CompilerParams(vmem_limit_bytes=8 << 20), name="split",
    )(
        lev.reshape(1), pltpu.with_memory_space_constraint(jnp.asarray(picks, bf16), pltpu.HBM),
        pltpu.with_memory_space_constraint(grid.reshape(levels, own, width), pltpu.HBM),
    )
    first = send(first, lambda c, i, j: (c, i + 2 * c - 1, j))
    corner_1 = send(corner_1, lambda c, i, j: (c, i + 2 * c - 1, j - 1))
    east = send(west, lambda c, i, j: (c, i, j - 1))
    second = send(second, lambda c, i, j: (c, i + 1 - 2 * c, j))
    corner_2 = send(corner_2, lambda c, i, j: (c, i + 1 - 2 * c, j - 1))

    heads_of = jnp.asarray(np.repeat(np.eye(heads, dtype=np.float32), width // heads, axis=1), bf16)
    quarter = edge // 2
    spots = [(r, c) for r in range(rows) for c in range(cols)]
    back = [i * edge + t for i in range(2) for t in range(quarter)]
    middle_to = [r * WO + c - EDGE if EDGE <= c < EDGE + WO else -1 for r, c in spots]
    border_to = [quarter + r * EDGE + c - EDGE - WO if c >= EDGE + WO else -1 for r, c in spots]
    returned_to = [i * quarter + r * EDGE + c if c < EDGE else -1 for i in range(2) for r, c in spots]
    tables = [
        gather_picks(levels, cols), one_hot(back, 2 * edge), one_hot(middle_to, edge), one_hot(border_to, edge),
        one_hot(returned_to, edge),
    ]
    groups, back, middle_to, border_to, returned_to, *shared = load(
        *(jnp.asarray(table, bf16) for table in tables),
        heads_of, logit_scale.reshape(1, heads), w_qkv, w_proj, w_up, w_down,
        gain_attn.reshape(1, width), gain_mlp.reshape(1, width),
    )

    outs = (shape(4 * edge, width), shape(4 * edge, width))
    alone, paired = call(gather_kernel, outs, 8)(place, groups, tokens, first, second, corner_1, corner_2, east)
    other = send(paired, lambda c, i, j: (1 - c, i, j))

    kv = [pltpu.VMEM((6 * edge, 2 * width), bf16)]
    border, returning = call(border_kernel, (shape(2 * edge, width), shape(edge, width)), 16, kv)(
        place, alone, paired, other, back, *shared
    )
    returned = send(returning, lambda c, i, j: (c, i, j + 1))
    partial = call(middle_kernel, shape(levels, own, width), 16, kv)(
        place, alone, paired, other, border, middle_to, border_to, *shared
    )
    out = call(place_kernel, shape(levels, own, width), 8)(place, partial, returned, returned_to)
    return out.reshape(levels, rows, cols, width)


def solution(mesh):
    placed = (P("lev", "lat", "lon", None), P(), P(), P(), P(), P(), P(), P())
    return jax.shard_map(
        per_device,
        mesh=mesh,
        in_specs=placed,
        out_specs=P("lev", "lat", "lon", None),
        check_vma=False,
    )
```

```python
import jax
import jax.numpy as jnp
import numpy as np
from jax import lax
from jax.experimental import pallas as pl
from jax.experimental.pallas import tpu as pltpu
from jax.sharding import PartitionSpec as P


WA = 6
WO = 12
EDGE = WO // 2
LOG2E = 1.4426950408889634
AXES = ("lev", "lat", "lon")


def send(array, target):
    sizes = [lax.axis_size(axis) for axis in AXES]
    route = []
    for lev in range(sizes[0]):
        for lat in range(sizes[1]):
            for lon in range(sizes[2]):
                at = [lev, lat, lon]
                to = [t % size for t, size in zip(target(lev, lat, lon), sizes)]
                flat = [(p[0] * sizes[1] + p[1]) * sizes[2] + p[2] for p in (at, to)]
                route.append(tuple(flat))
    return lax.ppermute(array, AXES, route)


def column_group(cols, first, last):
    own = [r * cols + c for r in range(WA) for c in range(first, last)]
    halo = [WA * cols + r * cols + c for r in range(WA) for c in range(first, last)]
    return own + halo


def one_hot(indices, size):
    table = np.zeros((len(indices), size), np.float32)
    for row, index in enumerate(indices):
        if index >= 0:
            table[row, index] = 1
    return jnp.asarray(table, jnp.bfloat16)


def gather_kernel(lev_ref, pick_ref, own_ref, first_ref, second_ref, alone_ref, paired_ref, west_ref, cross_ref):
    lev = lev_ref[0]
    kept = alone_ref.shape[0]
    edge = cross_ref.shape[0]
    for i, (level, out_ref) in enumerate(((lev, alone_ref), (1 - lev, paired_ref))):
        source = jnp.concatenate([own_ref[level], first_ref[level], second_ref[level]], 0)
        picked = jnp.dot(pick_ref[...], source, preferred_element_type=jnp.float32)
        picked = picked.astype(jnp.bfloat16)
        out_ref[...] = picked[:kept]
        west_ref[i * edge : (i + 1) * edge, :] = picked[kept:]
        if i == 1:
            cross_ref[...] = picked[kept:]


def load_kernel(*refs):
    count = len(refs) // 2
    sems = refs[-1]
    copies = [pltpu.make_async_copy(refs[i], refs[count + i], sems.at[i]) for i in range(count)]
    for copy in copies:
        copy.start()
    for copy in copies:
        copy.wait()


def load(*args):
    return pl.pallas_call(
        load_kernel,
        out_shape=tuple(jax.ShapeDtypeStruct(a.shape, a.dtype) for a in args),
        in_specs=[pl.BlockSpec(memory_space=pltpu.HBM)] * len(args),
        out_specs=(VMEM,) * len(args),
        scratch_shapes=[pltpu.SemaphoreType.DMA((len(args),))],
        compiler_params=pltpu.CompilerParams(vmem_limit_bytes=10 << 20),
        name="load",
    )(*(pltpu.with_memory_space_constraint(a, pltpu.HBM) for a in args))


def layer_norm(values, gain):
    mean = jnp.mean(values, axis=-1, keepdims=True)
    centred = values - mean
    spread = jnp.mean(centred * centred, axis=-1, keepdims=True)
    return centred * lax.rsqrt(spread + 1e-05) * gain


def split_squares(values):
    squares = values.astype(jnp.float32)
    squares = squares * squares
    high = squares.astype(jnp.bfloat16)
    low = (squares - high.astype(jnp.float32)).astype(jnp.bfloat16)
    return high, low


def contract_last(a, b):
    return lax.dot_general(a, b, (((1,), (1,)), ((), ())), preferred_element_type=jnp.float32)


def attend(query, keys, values, allowed, logit, heads_of):
    count, width = query.shape
    heads = heads_of.shape[0]
    size = width // heads
    pair = 2 * size
    high, low = split_squares(query)
    q_scale = contract_last(high, heads_of) + contract_last(low, heads_of)
    q_scale = lax.rsqrt(q_scale + 1e-06) * logit
    high, low = split_squares(keys)
    k_scale = contract_last(heads_of, high) + contract_last(heads_of, low)
    k_scale = lax.rsqrt(k_scale + 1e-06)
    lane = lax.broadcasted_iota(jnp.int32, (count, pair), 1)
    zero = jnp.zeros((count, pair), jnp.bfloat16)
    ones = jnp.ones((keys.shape[0], pair), jnp.bfloat16)
    parts = []
    for p in range(heads // 2):
        q = query[:, p * pair : (p + 1) * pair]
        k = keys[:, p * pair : (p + 1) * pair]
        v = jnp.concatenate([values[:, p * pair : (p + 1) * pair], ones], 1)
        both = jnp.concatenate([jnp.where(lane < size, q, zero), jnp.where(lane < size, zero, q)], 0)
        raw = contract_last(both, k)
        expd = []
        for side in range(2):
            h = 2 * p + side
            scores = raw[side * count : (side + 1) * count] * q_scale[:, h : h + 1] * k_scale[h : h + 1, :]
            expd.append((jnp.exp2(scores) * allowed).astype(jnp.bfloat16))
        mixed = jnp.dot(jnp.concatenate(expd, 0), v, preferred_element_type=jnp.float32)
        mixed = mixed[:, :pair] / mixed[:, pair:]
        parts.append(jnp.where(lane < size, mixed[:count], mixed[count:]).astype(jnp.bfloat16))
    return jnp.concatenate(parts, 1)


def allowed_keys(place_ref, queries, group):
    first = place_ref[3]
    shape = (queries, 2 * queries)
    row = lax.broadcasted_iota(jnp.int32, shape, 0)
    col = lax.broadcasted_iota(jnp.int32, shape, 1)
    row = lax.rem(row, group)
    col = lax.rem(col, 2 * group)
    quarter = group // 2
    q_half = jnp.where(row < quarter, 0, 1)
    k_half = jnp.where(col < quarter, 0, jnp.where(col < 2 * quarter, 1, jnp.where(col < 3 * quarter, first, 1 - first)))
    closed = jnp.where(k_half == 0, place_ref[1], place_ref[2])
    return jnp.where((q_half == k_half) & ((col < group) | (closed == 0)), 1.0, 0.0)


def run_windows(sources, query, place_ref, group, heads_ref, logit_ref, weights, kv_ref):
    qkv_ref, proj_ref, up_ref, down_ref, gain_attn_ref, gain_mlp_ref = weights
    width = proj_ref.shape[0]
    tokens = kv_ref.shape[0]
    span = tokens // 3
    count = span // 2
    kv = jnp.dot(sources, qkv_ref[:, width:], preferred_element_type=jnp.float32)
    kv_ref[...] = kv.astype(jnp.bfloat16)
    q = jnp.dot(query, qkv_ref[:, :width], preferred_element_type=jnp.float32).astype(jnp.bfloat16)
    own = allowed_keys(place_ref, count, group)
    logit = logit_ref[...] * LOG2E
    mixed = []
    for i, (first, last, allowed) in enumerate(((0, span, own), (span, tokens, jnp.concatenate([own, own], 1)))):
        keys = kv_ref[first:last, :width]
        values = kv_ref[first:last, width:]
        mixed.append(attend(q[i * count : (i + 1) * count], keys, values, allowed, logit, heads_ref[...]))
    mixed = jnp.concatenate(mixed, 0)
    attn_out = jnp.dot(mixed, proj_ref[...], preferred_element_type=jnp.float32)
    attn_out = attn_out.astype(jnp.bfloat16).astype(jnp.float32)
    settled = (query.astype(jnp.float32) + layer_norm(attn_out, gain_attn_ref[...])).astype(jnp.bfloat16)
    hidden = jnp.dot(settled, up_ref[...], preferred_element_type=jnp.float32)
    hidden = jax.nn.gelu(hidden, approximate=True).astype(jnp.bfloat16)
    down = jnp.dot(hidden, down_ref[...], preferred_element_type=jnp.float32)
    result = settled.astype(jnp.float32) + layer_norm(down, gain_mlp_ref[...])
    return result.astype(jnp.bfloat16)


def border_kernel(
    place_ref, alone_ref, paired_ref, other_ref, east_ref, cross_ref, pick_ref, back_ref, heads_ref, logit_ref,
    qkv_ref, proj_ref, up_ref, down_ref, gain_attn_ref, gain_mlp_ref, out_ref, return_ref, kv_ref,
):
    edge = cross_ref.shape[0]
    start = alone_ref.shape[0] - edge
    pieces = (
        alone_ref[start:, :], east_ref[:edge, :], paired_ref[start:, :], east_ref[edge:, :],
        other_ref[start:, :], cross_ref[...],
    )
    sources = jnp.concatenate(pieces, 0)
    query = [
        jnp.dot(pick_ref[...], sources[i * 2 * edge : (i + 1) * 2 * edge], preferred_element_type=jnp.float32)
        for i in range(2)
    ]
    query = jnp.concatenate(query, 0).astype(jnp.bfloat16)
    weights = (qkv_ref, proj_ref, up_ref, down_ref, gain_attn_ref, gain_mlp_ref)
    result = run_windows(sources, query, place_ref, edge // 2, heads_ref, logit_ref, weights, kv_ref)
    out_ref[...] = result
    back = jnp.dot(back_ref[...], result, preferred_element_type=jnp.float32)
    return_ref[...] = back.astype(jnp.bfloat16)


def middle_kernel(
    place_ref, alone_ref, paired_ref, other_ref, border_ref, middle_to_ref, border_to_ref, heads_ref, logit_ref,
    qkv_ref, proj_ref, up_ref, down_ref, gain_attn_ref, gain_mlp_ref, out_ref, kv_ref,
):
    lev = place_ref[0]
    span = kv_ref.shape[0] // 3
    count = span // 2
    sources = jnp.concatenate([alone_ref[:span, :], paired_ref[:span, :], other_ref[:span, :]], 0)
    query = jnp.concatenate([alone_ref[:count, :], paired_ref[:count, :]], 0)
    weights = (qkv_ref, proj_ref, up_ref, down_ref, gain_attn_ref, gain_mlp_ref)
    result = run_windows(sources, query, place_ref, count, heads_ref, logit_ref, weights, kv_ref)
    for i, level in enumerate((lev, 1 - lev)):
        placed = jnp.dot(middle_to_ref[...], result[i * count : (i + 1) * count], preferred_element_type=jnp.float32)
        placed += jnp.dot(border_to_ref[...], border_ref[i * count : (i + 1) * count, :], preferred_element_type=jnp.float32)
        out_ref[level] = placed.astype(jnp.bfloat16)


def place_kernel(place_ref, partial_ref, returned_ref, returned_to_ref, out_ref):
    lev = place_ref[0]
    own = partial_ref.shape[1]
    for i, level in enumerate((lev, 1 - lev)):
        placed = jnp.dot(
            returned_to_ref[i * own : (i + 1) * own, :], returned_ref[...], preferred_element_type=jnp.float32
        )
        row = lax.broadcasted_iota(jnp.int32, placed.shape, 0)
        mine = lax.rem(row, own // WA) >= EDGE
        out_ref[level] = jnp.where(mine, partial_ref[level], placed.astype(jnp.bfloat16))


VMEM = pl.BlockSpec(memory_space=pltpu.VMEM)
SMEM = pl.BlockSpec(memory_space=pltpu.SMEM)


def call(kernel, outs, megabytes, scratch=()):
    def run(place, *args):
        return pl.pallas_call(
            kernel,
            out_shape=outs,
            in_specs=[SMEM] + [VMEM] * len(args),
            out_specs=jax.tree.map(lambda _: VMEM, outs),
            scratch_shapes=list(scratch),
            compiler_params=pltpu.CompilerParams(vmem_limit_bytes=megabytes << 20),
        )(place, *args)

    return run


def per_device(grid, w_qkv, w_proj, w_up, w_down, logit_scale, gain_attn, gain_mlp):
    levels, rows, cols, width = grid.shape
    own = rows * cols
    half = own // 2
    edge = 2 * WA * EDGE
    heads = logit_scale.shape[0]
    bf16 = jnp.bfloat16

    def shape(*dims):
        return jax.ShapeDtypeStruct(dims, bf16)

    lev = lax.axis_index("lev").astype(jnp.int32)
    lat = lax.axis_index("lat")
    last = lax.axis_size("lat") - 1
    place = jnp.stack([lev, (lat == 0).astype(jnp.int32), (lat == last).astype(jnp.int32), lax.rem(lat, 2).astype(jnp.int32)])

    tokens = grid.reshape(levels, own, width)
    halves = grid.reshape(levels, 2, half, width)
    odd = lax.rem(lat, 2).astype(jnp.int32)
    sent_first = lax.dynamic_index_in_dim(halves, odd, 1, keepdims=False)
    sent_second = lax.dynamic_index_in_dim(halves, 1 - odd, 1, keepdims=False)
    first = send(sent_first, lambda c, i, j: (c, i - 1 + 2 * (i % 2), j))
    second = send(sent_second, lambda c, i, j: (c, i + 1 - 2 * (i % 2), j))

    groups = column_group(cols, EDGE, EDGE + WO) + column_group(cols, EDGE + WO, cols) + column_group(cols, 0, EDGE)
    heads_of = jnp.asarray(np.repeat(np.eye(heads, dtype=np.float32), width // heads, axis=1), bf16)
    quarter = edge // 2
    spots = [(r, c) for r in range(rows) for c in range(cols)]
    pick = [edge + t for t in range(quarter)] + list(range(quarter))
    back = [i * edge + t for i in range(2) for t in range(quarter)]
    middle_to = [r * WO + c - EDGE if EDGE <= c < EDGE + WO else -1 for r, c in spots]
    border_to = [quarter + r * EDGE + c - EDGE - WO if c >= EDGE + WO else -1 for r, c in spots]
    returned_to = [i * quarter + r * EDGE + c if c < EDGE else -1 for i in range(2) for r, c in spots]
    tokens, groups, pick, back, middle_to, border_to, returned_to, *shared = load(
        tokens, one_hot(groups, 2 * own), one_hot(pick, 2 * edge), one_hot(back, 2 * edge), one_hot(middle_to, edge),
        one_hot(border_to, edge), one_hot(returned_to, edge),
        heads_of, logit_scale.reshape(1, heads), w_qkv, w_proj, w_up, w_down,
        gain_attn.reshape(1, width), gain_mlp.reshape(1, width),
    )

    kept = 2 * own - edge
    outs = (shape(kept, width), shape(kept, width), shape(2 * edge, width), shape(edge, width))
    alone, paired, west, west_paired = call(gather_kernel, outs, 8)(place, groups, tokens, first, second)
    east = send(west, lambda c, i, j: (c, i, j - 1))
    cross = send(west_paired, lambda c, i, j: (1 - c, i, j - 1))
    other = send(paired, lambda c, i, j: (1 - c, i, j))

    kv = [pltpu.VMEM((6 * edge, 2 * width), bf16)]
    border, returning = call(border_kernel, (shape(2 * edge, width), shape(edge, width)), 16, kv)(
        place, alone, paired, other, east, cross, pick, back, *shared
    )
    returned = send(returning, lambda c, i, j: (c, i, j + 1))
    partial = call(middle_kernel, shape(levels, own, width), 16, kv)(
        place, alone, paired, other, border, middle_to, border_to, *shared
    )
    out = call(place_kernel, shape(levels, own, width), 8)(place, partial, returned, returned_to)
    return out.reshape(levels, rows, cols, width)


def solution(mesh):
    placed = (P("lev", "lat", "lon", None), P(), P(), P(), P(), P(), P(), P())
    return jax.shard_map(
        per_device,
        mesh=mesh,
        in_specs=placed,
        out_specs=P("lev", "lat", "lon", None),
        check_vma=False,
    )
```

```python
import jax
import jax.numpy as jnp
import numpy as np
from jax import lax
from jax.experimental import pallas as pl
from jax.experimental.pallas import tpu as pltpu
from jax.sharding import PartitionSpec as P


WA = 6
WO = 12
EDGE = WO // 2
LOG2E = 1.4426950408889634
AXES = ("lev", "lat", "lon")


def send(array, target):
    sizes = [lax.axis_size(axis) for axis in AXES]
    route = []
    for lev in range(sizes[0]):
        for lat in range(sizes[1]):
            for lon in range(sizes[2]):
                at = [lev, lat, lon]
                to = [t % size for t, size in zip(target(lev, lat, lon), sizes)]
                flat = [(p[0] * sizes[1] + p[1]) * sizes[2] + p[2] for p in (at, to)]
                route.append(tuple(flat))
    return lax.ppermute(array, AXES, route)


def column_group(cols, first, last):
    own = [r * cols + c for r in range(WA) for c in range(first, last)]
    halo = [WA * cols + r * cols + c for r in range(WA) for c in range(first, last)]
    return own + halo


def one_hot(indices, size):
    table = np.zeros((len(indices), size), np.float32)
    for row, index in enumerate(indices):
        if index >= 0:
            table[row, index] = 1
    return jnp.asarray(table, jnp.bfloat16)


def edge_rows(place_ref, which, kept, edge):
    odd = place_ref[4]
    return pl.ds(pl.multiple_of(kept + edge * (odd if which == 0 else 1 - odd), 8), edge)


def gather_kernel(
    place_ref, pick_ref, own_ref, first_ref, second_ref,
    alone_ref, paired_ref, swap_1_ref, swap_2_ref, cross_1_ref, cross_2_ref,
):
    lev = place_ref[0]
    edge = cross_1_ref.shape[0]
    kept = alone_ref.shape[0] - 2 * edge
    for i, (level, out_ref) in enumerate(((lev, alone_ref), (1 - lev, paired_ref))):
        source = jnp.concatenate([own_ref[level], first_ref[level], second_ref[level]], 0)
        picked = jnp.dot(pick_ref[...], source, preferred_element_type=jnp.float32)
        out_ref[...] = picked.astype(jnp.bfloat16)
        for which, swap_ref in enumerate((swap_1_ref, swap_2_ref)):
            swap_ref[i * edge : (i + 1) * edge, :] = out_ref[edge_rows(place_ref, which, kept, edge), :]
    for which, cross_ref in enumerate((cross_1_ref, cross_2_ref)):
        cross_ref[...] = paired_ref[edge_rows(place_ref, which, kept, edge), :]


def load_kernel(*refs):
    count = len(refs) // 2
    sems = refs[-1]
    copies = [pltpu.make_async_copy(refs[i], refs[count + i], sems.at[i]) for i in range(count)]
    for copy in copies:
        copy.start()
    for copy in copies:
        copy.wait()


def load(*args):
    return pl.pallas_call(
        load_kernel,
        out_shape=tuple(jax.ShapeDtypeStruct(a.shape, a.dtype) for a in args),
        in_specs=[pl.BlockSpec(memory_space=pltpu.HBM)] * len(args),
        out_specs=(VMEM,) * len(args),
        scratch_shapes=[pltpu.SemaphoreType.DMA((len(args),))],
        compiler_params=pltpu.CompilerParams(vmem_limit_bytes=10 << 20),
        name="load",
    )(*(pltpu.with_memory_space_constraint(a, pltpu.HBM) for a in args))


def layer_norm(values, gain):
    mean = jnp.mean(values, axis=-1, keepdims=True)
    centred = values - mean
    spread = jnp.mean(centred * centred, axis=-1, keepdims=True)
    return centred * lax.rsqrt(spread + 1e-05) * gain


def split_squares(values):
    squares = values.astype(jnp.float32)
    squares = squares * squares
    high = squares.astype(jnp.bfloat16)
    low = (squares - high.astype(jnp.float32)).astype(jnp.bfloat16)
    return high, low


def contract_last(a, b):
    return lax.dot_general(a, b, (((1,), (1,)), ((), ())), preferred_element_type=jnp.float32)


def attend(query, keys, values, allowed, logit, heads_of):
    count, width = query.shape
    heads = heads_of.shape[0]
    size = width // heads
    pair = 2 * size
    high, low = split_squares(query)
    q_scale = contract_last(high, heads_of) + contract_last(low, heads_of)
    q_scale = lax.rsqrt(q_scale + 1e-06) * logit
    high, low = split_squares(keys)
    k_scale = contract_last(heads_of, high) + contract_last(heads_of, low)
    k_scale = lax.rsqrt(k_scale + 1e-06)
    lane = lax.broadcasted_iota(jnp.int32, (count, pair), 1)
    zero = jnp.zeros((count, pair), jnp.bfloat16)
    ones = jnp.ones((keys.shape[0], pair), jnp.bfloat16)
    parts = []
    for p in range(heads // 2):
        q = query[:, p * pair : (p + 1) * pair]
        k = keys[:, p * pair : (p + 1) * pair]
        v = jnp.concatenate([values[:, p * pair : (p + 1) * pair], ones], 1)
        both = jnp.concatenate([jnp.where(lane < size, q, zero), jnp.where(lane < size, zero, q)], 0)
        raw = contract_last(both, k)
        expd = []
        for side in range(2):
            h = 2 * p + side
            scores = raw[side * count : (side + 1) * count] * q_scale[:, h : h + 1] * k_scale[h : h + 1, :]
            expd.append((jnp.exp2(scores) * allowed).astype(jnp.bfloat16))
        mixed = jnp.dot(jnp.concatenate(expd, 0), v, preferred_element_type=jnp.float32)
        mixed = mixed[:, :pair] / mixed[:, pair:]
        parts.append(jnp.where(lane < size, mixed[:count], mixed[count:]).astype(jnp.bfloat16))
    return jnp.concatenate(parts, 1)


def allowed_keys(place_ref, queries, keys, group, sets):
    first = place_ref[3]
    shape = (queries, keys)
    row = lax.broadcasted_iota(jnp.int32, shape, 0)
    col = lax.broadcasted_iota(jnp.int32, shape, 1)
    q_set = row // group
    k_set = lax.rem(col // (2 * group), sets)
    row = lax.rem(row, group)
    col = lax.rem(col, 2 * group)
    quarter = group // 2
    q_half = jnp.where(row < quarter, 0, 1)
    k_half = jnp.where(col < quarter, 0, jnp.where(col < 2 * quarter, 1, jnp.where(col < 3 * quarter, first, 1 - first)))
    closed = jnp.where(k_half == 0, place_ref[1], place_ref[2])
    return jnp.where((q_half == k_half) & (q_set == k_set) & ((col < group) | (closed == 0)), 1.0, 0.0)


def run_windows(sources, query, place_ref, group, sets, heads_ref, logit_ref, weights, kv_ref):
    qkv_ref, proj_ref, up_ref, down_ref, gain_attn_ref, gain_mlp_ref = weights
    width = proj_ref.shape[0]
    tokens = kv_ref.shape[0]
    span = tokens // 3
    count = query.shape[0] // 2
    kv = jnp.dot(sources, qkv_ref[:, width:], preferred_element_type=jnp.float32)
    kv_ref[...] = kv.astype(jnp.bfloat16)
    q = jnp.dot(query, qkv_ref[:, :width], preferred_element_type=jnp.float32).astype(jnp.bfloat16)
    own = allowed_keys(place_ref, count, span, group, sets)
    logit = logit_ref[...] * LOG2E
    mixed = []
    for i, (first, last, allowed) in enumerate(((0, span, own), (span, tokens, jnp.concatenate([own, own], 1)))):
        keys = kv_ref[first:last, :width]
        values = kv_ref[first:last, width:]
        mixed.append(attend(q[i * count : (i + 1) * count], keys, values, allowed, logit, heads_ref[...]))
    mixed = jnp.concatenate(mixed, 0)
    attn_out = jnp.dot(mixed, proj_ref[...], preferred_element_type=jnp.float32)
    attn_out = attn_out.astype(jnp.bfloat16).astype(jnp.float32)
    settled = (query.astype(jnp.float32) + layer_norm(attn_out, gain_attn_ref[...])).astype(jnp.bfloat16)
    hidden = jnp.dot(settled, up_ref[...], preferred_element_type=jnp.float32)
    hidden = jax.nn.gelu(hidden, approximate=True).astype(jnp.bfloat16)
    down = jnp.dot(hidden, down_ref[...], preferred_element_type=jnp.float32)
    result = settled.astype(jnp.float32) + layer_norm(down, gain_mlp_ref[...])
    return result.astype(jnp.bfloat16)


def middle_kernel(
    place_ref, alone_ref, paired_ref, other_ref, heads_ref, logit_ref,
    qkv_ref, proj_ref, up_ref, down_ref, gain_attn_ref, gain_mlp_ref, out_ref, kv_ref,
):
    span = kv_ref.shape[0] // 3
    count = span // 2
    sources = jnp.concatenate([alone_ref[:span, :], paired_ref[:span, :], other_ref[:span, :]], 0)
    query = jnp.concatenate([alone_ref[:count, :], paired_ref[:count, :]], 0)
    weights = (qkv_ref, proj_ref, up_ref, down_ref, gain_attn_ref, gain_mlp_ref)
    out_ref[...] = run_windows(sources, query, place_ref, count, 1, heads_ref, logit_ref, weights, kv_ref)


def border_kernel(
    place_ref, alone_ref, paired_ref, other_ref, swap_1_ref, swap_2_ref, cross_1_ref, cross_2_ref, middle_ref,
    pick_ref, middle_to_ref, border_to_ref, heads_ref, logit_ref,
    qkv_ref, proj_ref, up_ref, down_ref, gain_attn_ref, gain_mlp_ref, out_ref, kv_ref,
):
    lev = place_ref[0]
    edge = cross_1_ref.shape[0]
    kept = alone_ref.shape[0] - 2 * edge
    pieces = []
    for i, ref in enumerate((alone_ref, paired_ref, other_ref)):
        pieces += [ref[edge_rows(place_ref, which, kept, edge), :] for which in range(2)]
        if i < 2:
            pieces += [swap[i * edge : (i + 1) * edge, :] for swap in (swap_1_ref, swap_2_ref)]
        else:
            pieces += [cross_1_ref[...], cross_2_ref[...]]
    sources = jnp.concatenate(pieces, 0)
    query = [
        jnp.dot(pick_ref[...], sources[i * 4 * edge : i * 4 * edge + 2 * edge], preferred_element_type=jnp.float32)
        for i in range(2)
    ]
    query = jnp.concatenate(query, 0).astype(jnp.bfloat16)
    weights = (qkv_ref, proj_ref, up_ref, down_ref, gain_attn_ref, gain_mlp_ref)
    result = run_windows(sources, query, place_ref, edge // 2, 2, heads_ref, logit_ref, weights, kv_ref)
    border_to = border_to_ref[place_ref[4]]
    for i, level in enumerate((lev, 1 - lev)):
        placed = jnp.dot(middle_to_ref[...], middle_ref[i * edge : (i + 1) * edge, :], preferred_element_type=jnp.float32)
        placed += jnp.dot(border_to, result[i * edge : (i + 1) * edge], preferred_element_type=jnp.float32)
        out_ref[level] = placed.astype(jnp.bfloat16)


VMEM = pl.BlockSpec(memory_space=pltpu.VMEM)
SMEM = pl.BlockSpec(memory_space=pltpu.SMEM)


def call(kernel, outs, megabytes, scratch=()):
    def run(place, *args):
        return pl.pallas_call(
            kernel,
            out_shape=outs,
            in_specs=[SMEM] + [VMEM] * len(args),
            out_specs=jax.tree.map(lambda _: VMEM, outs),
            scratch_shapes=list(scratch),
            compiler_params=pltpu.CompilerParams(vmem_limit_bytes=megabytes << 20),
        )(place, *args)

    return run


def per_device(grid, w_qkv, w_proj, w_up, w_down, logit_scale, gain_attn, gain_mlp):
    levels, rows, cols, width = grid.shape
    own = rows * cols
    half = own // 2
    edge = 2 * WA * EDGE
    heads = logit_scale.shape[0]
    bf16 = jnp.bfloat16

    def shape(*dims):
        return jax.ShapeDtypeStruct(dims, bf16)

    lev = lax.axis_index("lev").astype(jnp.int32)
    lat = lax.axis_index("lat")
    last = lax.axis_size("lat") - 1
    place = jnp.stack([lev, (lat == 0).astype(jnp.int32), (lat == last).astype(jnp.int32), 1 - lax.rem(lat, 2).astype(jnp.int32), lax.rem(lax.axis_index("lon"), 2).astype(jnp.int32)])

    tokens = grid.reshape(levels, own, width)
    halves = grid.reshape(levels, 2, half, width)
    even = 1 - lax.rem(lat, 2).astype(jnp.int32)
    sent_first = lax.dynamic_index_in_dim(halves, even, 1, keepdims=False)
    sent_second = lax.dynamic_index_in_dim(halves, 1 - even, 1, keepdims=False)
    first = send(sent_first, lambda c, i, j: (c, i + 1 - 2 * (i % 2), j))
    second = send(sent_second, lambda c, i, j: (c, i - 1 + 2 * (i % 2), j))

    groups = column_group(cols, EDGE, EDGE + WO) + column_group(cols, EDGE + WO, cols) + column_group(cols, 0, EDGE)
    heads_of = jnp.asarray(np.repeat(np.eye(heads, dtype=np.float32), width // heads, axis=1), bf16)
    quarter = edge // 2
    spots = [(r, c) for r in range(rows) for c in range(cols)]
    pick = list(range(quarter)) + [edge + t for t in range(quarter)]
    middle_to = [r * WO + c - EDGE if EDGE <= c < EDGE + WO else -1 for r, c in spots]

    def edge_spot(odd, r, c):
        if EDGE <= c < EDGE + WO:
            return -1
        west = c < EDGE
        return quarter * (west != odd) + r * EDGE + (c if west else c - EDGE - WO)

    border_to = [one_hot([edge_spot(odd, r, c) for r, c in spots], edge) for odd in (False, True)]
    tokens, groups, pick, middle_to, border_to, *shared = load(
        tokens, one_hot(groups, 2 * own), one_hot(pick, 2 * edge), one_hot(middle_to, edge), jnp.stack(border_to),
        heads_of, logit_scale.reshape(1, heads), w_qkv, w_proj, w_up, w_down,
        gain_attn.reshape(1, width), gain_mlp.reshape(1, width),
    )

    both = shape(2 * edge, width)
    outs = (shape(2 * own, width), shape(2 * own, width), both, both, shape(edge, width), shape(edge, width))
    alone, paired, swap_1, swap_2, cross_1, cross_2 = call(gather_kernel, outs, 8)(place, groups, tokens, first, second)
    swap_1 = send(swap_1, lambda c, i, j: (c, i, j + 1 - 2 * (j % 2)))
    swap_2 = send(swap_2, lambda c, i, j: (c, i, j - 1 + 2 * (j % 2)))
    other = send(paired, lambda c, i, j: (1 - c, i, j))
    cross_1 = send(cross_1, lambda c, i, j: (1 - c, i, j + 1 - 2 * (j % 2)))
    cross_2 = send(cross_2, lambda c, i, j: (1 - c, i, j - 1 + 2 * (j % 2)))

    kv = [pltpu.VMEM((6 * edge, 2 * width), bf16)]
    middle = call(middle_kernel, both, 16, kv)(place, alone, paired, other, *shared)
    kv = [pltpu.VMEM((12 * edge, 2 * width), bf16)]
    out = call(border_kernel, shape(levels, own, width), 20, kv)(
        place, alone, paired, other, swap_1, swap_2, cross_1, cross_2, middle, pick, middle_to, border_to, *shared
    )
    return out.reshape(levels, rows, cols, width)


def solution(mesh):
    placed = (P("lev", "lat", "lon", None), P(), P(), P(), P(), P(), P(), P())
    return jax.shard_map(
        per_device,
        mesh=mesh,
        in_specs=placed,
        out_specs=P("lev", "lat", "lon", None),
        check_vma=False,
    )
```

```python
import jax
import jax.numpy as jnp
import numpy as np
from jax import lax
from jax.experimental import pallas as pl
from jax.experimental.pallas import tpu as pltpu
from jax.sharding import PartitionSpec as P


WA = 6
WO = 12
EDGE = WO // 2
LOG2E = 1.4426950408889634
AXES = ("lev", "lat", "lon")


def send(array, target):
    sizes = [lax.axis_size(axis) for axis in AXES]
    route = []
    for lev in range(sizes[0]):
        for lat in range(sizes[1]):
            for lon in range(sizes[2]):
                at = [lev, lat, lon]
                to = [t % size for t, size in zip(target(lev, lat, lon), sizes)]
                flat = [(p[0] * sizes[1] + p[1]) * sizes[2] + p[2] for p in (at, to)]
                route.append(tuple(flat))
    return lax.ppermute(array, AXES, route)


def column_group(cols, first, last):
    own = [r * cols + c for r in range(WA) for c in range(first, last)]
    halo = [WA * cols + r * cols + c for r in range(WA) for c in range(first, last)]
    return own + halo


def one_hot(indices, size):
    table = np.zeros((len(indices), size), np.float32)
    for row, index in enumerate(indices):
        if index >= 0:
            table[row, index] = 1
    return jnp.asarray(table, jnp.bfloat16)


def edge_rows(place_ref, which, kept, edge):
    west = place_ref[4]
    return pl.ds(pl.multiple_of(kept + edge * (west if which == 0 else 1 - west), 8), edge)


def gather_kernel(
    place_ref, pick_ref, own_ref, first_ref, second_ref,
    alone_ref, paired_ref, swap_1_ref, swap_2_ref,
):
    lev = place_ref[0]
    edge = swap_1_ref.shape[0] // 2
    kept = alone_ref.shape[0] - 2 * edge
    for i, (level, out_ref) in enumerate(((lev, alone_ref), (1 - lev, paired_ref))):
        source = jnp.concatenate([own_ref[level], first_ref[level], second_ref[level]], 0)
        picked = jnp.dot(pick_ref[...], source, preferred_element_type=jnp.float32)
        out_ref[...] = picked.astype(jnp.bfloat16)
        for which, swap_ref in enumerate((swap_1_ref, swap_2_ref)):
            swap_ref[i * edge : (i + 1) * edge, :] = out_ref[edge_rows(place_ref, which, kept, edge), :]


def load_kernel(*refs):
    count = len(refs) // 2
    sems = refs[-1]
    copies = [pltpu.make_async_copy(refs[i], refs[count + i], sems.at[i]) for i in range(count)]
    for copy in copies:
        copy.start()
    for copy in copies:
        copy.wait()


def load(*args):
    return pl.pallas_call(
        load_kernel,
        out_shape=tuple(jax.ShapeDtypeStruct(a.shape, a.dtype) for a in args),
        in_specs=[pl.BlockSpec(memory_space=pltpu.HBM)] * len(args),
        out_specs=(VMEM,) * len(args),
        scratch_shapes=[pltpu.SemaphoreType.DMA((len(args),))],
        compiler_params=pltpu.CompilerParams(vmem_limit_bytes=10 << 20),
        name="load",
    )(*(pltpu.with_memory_space_constraint(a, pltpu.HBM) for a in args))


def layer_norm(values, gain):
    mean = jnp.mean(values, axis=-1, keepdims=True)
    centred = values - mean
    spread = jnp.mean(centred * centred, axis=-1, keepdims=True)
    return centred * lax.rsqrt(spread + 1e-05) * gain


def split_squares(values):
    squares = values.astype(jnp.float32)
    squares = squares * squares
    high = squares.astype(jnp.bfloat16)
    low = (squares - high.astype(jnp.float32)).astype(jnp.bfloat16)
    return high, low


def contract_last(a, b):
    return lax.dot_general(a, b, (((1,), (1,)), ((), ())), preferred_element_type=jnp.float32)


def attend(query, keys, values, allowed, logit, heads_of):
    count, width = query.shape
    heads = heads_of.shape[0]
    size = width // heads
    pair = 2 * size
    high, low = split_squares(query)
    q_scale = contract_last(high, heads_of) + contract_last(low, heads_of)
    q_scale = lax.rsqrt(q_scale + 1e-06) * logit
    high, low = split_squares(keys)
    k_scale = contract_last(heads_of, high) + contract_last(heads_of, low)
    k_scale = lax.rsqrt(k_scale + 1e-06)
    lane = lax.broadcasted_iota(jnp.int32, (count, pair), 1)
    zero = jnp.zeros((count, pair), jnp.bfloat16)
    ones = jnp.ones((keys.shape[0], pair), jnp.bfloat16)
    parts = []
    for p in range(heads // 2):
        q = query[:, p * pair : (p + 1) * pair]
        k = keys[:, p * pair : (p + 1) * pair]
        v = jnp.concatenate([values[:, p * pair : (p + 1) * pair], ones], 1)
        both = jnp.concatenate([jnp.where(lane < size, q, zero), jnp.where(lane < size, zero, q)], 0)
        raw = contract_last(both, k)
        expd = []
        for side in range(2):
            h = 2 * p + side
            scores = raw[side * count : (side + 1) * count] * q_scale[:, h : h + 1] * k_scale[h : h + 1, :]
            expd.append((jnp.exp2(scores) * allowed).astype(jnp.bfloat16))
        mixed = jnp.dot(jnp.concatenate(expd, 0), v, preferred_element_type=jnp.float32)
        mixed = mixed[:, :pair] / mixed[:, pair:]
        parts.append(jnp.where(lane < size, mixed[:count], mixed[count:]).astype(jnp.bfloat16))
    return jnp.concatenate(parts, 1)


def allowed_keys(place_ref, queries, keys, group, sets):
    first = place_ref[3]
    shape = (queries, keys)
    row = lax.broadcasted_iota(jnp.int32, shape, 0)
    col = lax.broadcasted_iota(jnp.int32, shape, 1)
    q_set = row // group
    k_set = lax.rem(col // (2 * group), sets)
    row = lax.rem(row, group)
    col = lax.rem(col, 2 * group)
    quarter = group // 2
    q_half = jnp.where(row < quarter, 0, 1)
    k_half = jnp.where(col < quarter, 0, jnp.where(col < 2 * quarter, 1, jnp.where(col < 3 * quarter, first, 1 - first)))
    closed = jnp.where(k_half == 0, place_ref[1], place_ref[2])
    return jnp.where((q_half == k_half) & (q_set == k_set) & ((col < group) | (closed == 0)), 1.0, 0.0)


def run_windows(sources, query, place_ref, group, sets, heads_ref, logit_ref, weights, kv_ref):
    qkv_ref, proj_ref, up_ref, down_ref, gain_attn_ref, gain_mlp_ref = weights
    width = proj_ref.shape[0]
    tokens = kv_ref.shape[0]
    span = tokens // 3
    count = query.shape[0] // 2
    kv = jnp.dot(sources, qkv_ref[:, width:], preferred_element_type=jnp.float32)
    kv_ref[...] = kv.astype(jnp.bfloat16)
    q = jnp.dot(query, qkv_ref[:, :width], preferred_element_type=jnp.float32).astype(jnp.bfloat16)
    own = allowed_keys(place_ref, count, span, group, sets)
    logit = logit_ref[...] * LOG2E
    mixed = []
    for i, (first, last, allowed) in enumerate(((0, span, own), (span, tokens, jnp.concatenate([own, own], 1)))):
        keys = kv_ref[first:last, :width]
        values = kv_ref[first:last, width:]
        mixed.append(attend(q[i * count : (i + 1) * count], keys, values, allowed, logit, heads_ref[...]))
    mixed = jnp.concatenate(mixed, 0)
    attn_out = jnp.dot(mixed, proj_ref[...], preferred_element_type=jnp.float32)
    attn_out = attn_out.astype(jnp.bfloat16).astype(jnp.float32)
    settled = (query.astype(jnp.float32) + layer_norm(attn_out, gain_attn_ref[...])).astype(jnp.bfloat16)
    hidden = jnp.dot(settled, up_ref[...], preferred_element_type=jnp.float32)
    hidden = jax.nn.gelu(hidden, approximate=True).astype(jnp.bfloat16)
    down = jnp.dot(hidden, down_ref[...], preferred_element_type=jnp.float32)
    result = settled.astype(jnp.float32) + layer_norm(down, gain_mlp_ref[...])
    return result.astype(jnp.bfloat16)


def middle_kernel(
    place_ref, alone_ref, paired_ref, other_ref, heads_ref, logit_ref,
    qkv_ref, proj_ref, up_ref, down_ref, gain_attn_ref, gain_mlp_ref, out_ref, kv_ref,
):
    span = kv_ref.shape[0] // 3
    count = span // 2
    sources = jnp.concatenate([alone_ref[:span, :], paired_ref[:span, :], other_ref[:span, :]], 0)
    query = jnp.concatenate([alone_ref[:count, :], paired_ref[:count, :]], 0)
    weights = (qkv_ref, proj_ref, up_ref, down_ref, gain_attn_ref, gain_mlp_ref)
    out_ref[...] = run_windows(sources, query, place_ref, count, 1, heads_ref, logit_ref, weights, kv_ref)


def border_kernel(
    place_ref, alone_ref, paired_ref, other_ref, swap_1_ref, swap_2_ref, cross_ref, middle_ref,
    pick_ref, middle_to_ref, border_to_ref, heads_ref, logit_ref,
    qkv_ref, proj_ref, up_ref, down_ref, gain_attn_ref, gain_mlp_ref, out_ref, kv_ref,
):
    lev = place_ref[0]
    edge = cross_ref.shape[0] // 2
    kept = alone_ref.shape[0] - 2 * edge
    pieces = []
    for i, ref in enumerate((alone_ref, paired_ref, other_ref)):
        pieces += [ref[edge_rows(place_ref, which, kept, edge), :] for which in range(2)]
        if i < 2:
            pieces += [swap[i * edge : (i + 1) * edge, :] for swap in (swap_1_ref, swap_2_ref)]
        else:
            pieces += [cross_ref[...]]
    sources = jnp.concatenate(pieces, 0)
    query = [
        jnp.dot(pick_ref[...], sources[i * 4 * edge : i * 4 * edge + 2 * edge], preferred_element_type=jnp.float32)
        for i in range(2)
    ]
    query = jnp.concatenate(query, 0).astype(jnp.bfloat16)
    weights = (qkv_ref, proj_ref, up_ref, down_ref, gain_attn_ref, gain_mlp_ref)
    result = run_windows(sources, query, place_ref, edge // 2, 2, heads_ref, logit_ref, weights, kv_ref)
    border_to = border_to_ref[place_ref[4]]
    for i, level in enumerate((lev, 1 - lev)):
        placed = jnp.dot(middle_to_ref[...], middle_ref[i * edge : (i + 1) * edge, :], preferred_element_type=jnp.float32)
        placed += jnp.dot(border_to, result[i * edge : (i + 1) * edge], preferred_element_type=jnp.float32)
        out_ref[level] = placed.astype(jnp.bfloat16)


VMEM = pl.BlockSpec(memory_space=pltpu.VMEM)
SMEM = pl.BlockSpec(memory_space=pltpu.SMEM)


def call(kernel, outs, megabytes, scratch=()):
    def run(place, *args):
        return pl.pallas_call(
            kernel,
            out_shape=outs,
            in_specs=[SMEM] + [VMEM] * len(args),
            out_specs=jax.tree.map(lambda _: VMEM, outs),
            scratch_shapes=list(scratch),
            compiler_params=pltpu.CompilerParams(vmem_limit_bytes=megabytes << 20),
        )(place, *args)

    return run


def per_device(grid, w_qkv, w_proj, w_up, w_down, logit_scale, gain_attn, gain_mlp):
    levels, rows, cols, width = grid.shape
    own = rows * cols
    half = own // 2
    edge = 2 * WA * EDGE
    heads = logit_scale.shape[0]
    bf16 = jnp.bfloat16

    def shape(*dims):
        return jax.ShapeDtypeStruct(dims, bf16)

    lev = lax.axis_index("lev").astype(jnp.int32)
    lat = lax.axis_index("lat")
    last = lax.axis_size("lat") - 1
    place = jnp.stack([lev, (lat == 0).astype(jnp.int32), (lat == last).astype(jnp.int32), 1 - lax.rem(lat, 2).astype(jnp.int32), 1 - lax.rem(lax.axis_index("lon"), 2).astype(jnp.int32)])

    tokens = grid.reshape(levels, own, width)
    halves = grid.reshape(levels, 2, half, width)
    even = 1 - lax.rem(lat, 2).astype(jnp.int32)
    sent_first = lax.dynamic_index_in_dim(halves, even, 1, keepdims=False)
    sent_second = lax.dynamic_index_in_dim(halves, 1 - even, 1, keepdims=False)
    first = send(sent_first, lambda c, i, j: (c, i + 1 - 2 * (i % 2), j))
    second = send(sent_second, lambda c, i, j: (c, i - 1 + 2 * (i % 2), j))

    groups = column_group(cols, EDGE, EDGE + WO) + column_group(cols, EDGE + WO, cols) + column_group(cols, 0, EDGE)
    heads_of = jnp.asarray(np.repeat(np.eye(heads, dtype=np.float32), width // heads, axis=1), bf16)
    quarter = edge // 2
    spots = [(r, c) for r in range(rows) for c in range(cols)]
    pick = list(range(quarter)) + [edge + t for t in range(quarter)]
    middle_to = [r * WO + c - EDGE if EDGE <= c < EDGE + WO else -1 for r, c in spots]

    def edge_spot(west_first, r, c):
        if EDGE <= c < EDGE + WO:
            return -1
        west = c < EDGE
        return quarter * (west != west_first) + r * EDGE + (c if west else c - EDGE - WO)

    border_to = [one_hot([edge_spot(side, r, c) for r, c in spots], edge) for side in (False, True)]
    tokens, groups, pick, middle_to, border_to, *shared = load(
        tokens, one_hot(groups, 2 * own), one_hot(pick, 2 * edge), one_hot(middle_to, edge), jnp.stack(border_to),
        heads_of, logit_scale.reshape(1, heads), w_qkv, w_proj, w_up, w_down,
        gain_attn.reshape(1, width), gain_mlp.reshape(1, width),
    )

    both = shape(2 * edge, width)
    outs = (shape(2 * own, width), shape(2 * own, width), both, both)
    alone, paired, swap_1, swap_2 = call(gather_kernel, outs, 8)(place, groups, tokens, first, second)
    swap_1 = send(swap_1, lambda c, i, j: (c, i, j - 1 + 2 * (j % 2)))
    swap_2 = send(swap_2, lambda c, i, j: (c, i, j + 1 - 2 * (j % 2)))
    other = send(paired, lambda c, i, j: (1 - c, i, j))
    cross = send(jnp.concatenate([swap_1[edge:], swap_2[edge:]], 0), lambda c, i, j: (1 - c, i, j))

    kv = [pltpu.VMEM((6 * edge, 2 * width), bf16)]
    middle = call(middle_kernel, both, 16, kv)(place, alone, paired, other, *shared)
    kv = [pltpu.VMEM((12 * edge, 2 * width), bf16)]
    out = call(border_kernel, shape(levels, own, width), 20, kv)(
        place, alone, paired, other, swap_1, swap_2, cross, middle, pick, middle_to, border_to, *shared
    )
    return out.reshape(levels, rows, cols, width)


def solution(mesh):
    placed = (P("lev", "lat", "lon", None), P(), P(), P(), P(), P(), P(), P())
    return jax.shard_map(
        per_device,
        mesh=mesh,
        in_specs=placed,
        out_specs=P("lev", "lat", "lon", None),
        check_vma=False,
    )
```
